32 devices in a mesh: gx: 2 (over y), gy: 4 (over z), gz: 4 (over x, core).
Axes of the slice: x: 2, y: 2, z: 4, core: 2. Of those that a mesh axis runs over, the one named last changes fastest.
Arguments:
- tokens: bfloat16 [512, 6144], P(('gx', 'gy'), 'gz'), may hold values from -6 to 6
- grad_out: bfloat16 [512, 6144], P(('gx', 'gy'), 'gz'), may hold values from -1.5 to 1.5
- w_in: bfloat16 [6144, 12288], P('gz', ('gy', 'gx')), may hold values from -0.078125 to 0.078125
- w_out: bfloat16 [12288, 6144], P(('gy', 'gx'), 'gz'), may hold values from -0.0546875 to 0.0546875
Outputs:
- mlp_out: bfloat16 [512, 6144], P(('gx', 'gy'), 'gz')
- tok_grad: bfloat16 [512, 6144], P(('gx', 'gy'), 'gz')
- win_grad: float32 [6144, 12288], P('gz', ('gy', 'gx'))
- wout_grad: float32 [12288, 6144], P(('gy', 'gx'), 'gz')
The draws below stay inside these ranges and needn't reach their ends.
All inputs are finite; a program needn't handle non-finite values.
Results may differ from the reference program's by a relative error of at most 0.01.
Values may be sent and summed in bfloat16 or wider, within the bound.
A program may use at most 128 MiB of HBM per device.

```python
import math
import jax
import jax.numpy as jnp
from jax import lax

D = 6144
FF = 12288
ROWS = 256
TOKENS = 512
N_GX = 2


def shard_levels(own_key, dims, shards, least, high):
    factor_of, own = 1.0, jax.random.fold_in(own_key, 6)
    for position, parts in shards:
        draws = jnp.exp(jax.random.uniform(jax.random.fold_in(own, position), (parts,), jnp.float32, least / len(shards), high / len(shards)))
        factor_of = factor_of * jnp.repeat(draws, dims[position] // parts).reshape([-1 if axis == position else 1 for axis in range(len(dims))])
    return factor_of


def centred(own_key, dims, spread, bound, shards=(), held_as=jnp.bfloat16):
    array = spread * jax.random.normal(own_key, dims, jnp.float32)
    if shards:
        array = array * shard_levels(own_key, dims, shards, -0.22, 0.18)
    return jnp.clip(array, -bound, bound).astype(held_as)


def setup_inputs(seed: int = 0) -> dict:
    keys = jax.random.split(jax.random.key(seed), 5)
    tokens = centred(keys[0], (TOKENS, D), 1.0, 6.0, ((0, 8), (1, 4)))
    grad_out = centred(keys[1], (TOKENS, D), 0.25, 1.5, ((0, 8), (1, 4)))
    w_in = centred(keys[2], (D, FF), D ** -0.5, 0.078125, ((0, 4), (1, 8)))
    w_out = centred(keys[3], (FF, D), FF ** -0.5, 0.0546875, ((0, 8), (1, 4)))
    return {"tokens": tokens, "grad_out": grad_out, "w_in": w_in, "w_out": w_out}


def gelu_slope(values):
    cdf = 0.5 * (1.0 + jax.scipy.special.erf(values * 0.7071067811865476))
    density = jnp.exp(-0.5 * values * values) * 0.3989422804014327
    return cdf + values * density

def reference(tokens, grad_out, w_in, w_out):
    block_scale = 1.0 / math.sqrt(ROWS)
    pre = jnp.dot(tokens, w_in, preferred_element_type=jnp.float32)
    act = jax.nn.gelu(pre, approximate=False).astype(jnp.bfloat16)
    mlp_out = jnp.dot(act, w_out, preferred_element_type=jnp.float32).astype(jnp.bfloat16)
    d_act = jnp.dot(grad_out, w_out.T, preferred_element_type=jnp.float32)
    d_pre = (d_act * gelu_slope(pre)).astype(jnp.bfloat16)
    tok_grad = jnp.dot(d_pre, w_in.T, preferred_element_type=jnp.float32).astype(jnp.bfloat16)
    wout_grad = jnp.zeros((FF, D), jnp.float32)
    win_grad = jnp.zeros((D, FF), jnp.float32)
    for block in range(N_GX):
        lower = block * ROWS
        part_out = (jnp.dot(act[lower:lower + ROWS].T, grad_out[lower:lower + ROWS], preferred_element_type=jnp.float32) * block_scale).astype(jnp.bfloat16)
        part_in = (jnp.dot(tokens[lower:lower + ROWS].T, d_pre[lower:lower + ROWS], preferred_element_type=jnp.float32) * block_scale).astype(jnp.bfloat16)
        part_out = lax.optimization_barrier(part_out)
        part_in = lax.optimization_barrier(part_in)
        wout_grad = wout_grad + part_out.astype(jnp.float32)
        win_grad = win_grad + part_in.astype(jnp.float32)
    return (mlp_out, tok_grad, win_grad, wout_grad)
```

```python
import functools
import math

import jax
import jax.numpy as jnp
from jax import lax
from jax.experimental import pallas as pl
from jax.experimental.pallas import tpu as pltpu
from jax.sharding import PartitionSpec as P

MESH = pl.DeviceIdType.MESH
F32, BF16 = jnp.float32, jnp.bfloat16


def contract(left, right, dims):
    return lax.dot_general(left, right, (dims, ((), ())), preferred_element_type=F32)


def ring_kernel(
    nx, ny, nz,
    tok_ref, grad_ref, win_ref, wout_ref,
    mlp_ref, tgrad_ref, tok_out, grad_out, act_out, dpre_out,
    rows_all, win, wout, part, part_in, hid_all, send_out, own, fold_in, fold, last_in,
    local, a_z, a_x, b_sem, c_sem, d_x, d_z,
):
    x, y, z = lax.axis_index("gx"), lax.axis_index("gy"), lax.axis_index("gz")
    t, width = tok_ref.shape
    hidden = win_ref.shape[1]
    rows = ny * t
    slab = rows // nz
    sends = []

    def block(e):
        return lax.rem(x - e + nx, nx)

    def peer(me, d, n):
        return lax.rem(me + d, n)

    def source(me, d, n):
        return lax.rem(me - d + n, n)

    def remote(src, dst, sems, index, device):
        return pltpu.make_async_remote_copy(
            src_ref=src, dst_ref=dst, send_sem=sems.at[(0, *index)],
            recv_sem=sems.at[(1, *index)], device_id=device, device_id_type=MESH,
        )

    def send(*args):
        copy = remote(*args)
        copy.start()
        sends.append(copy)

    stage = [
        pltpu.make_async_copy(tok_ref, rows_all.at[0, x, y], local.at[0]),
        pltpu.make_async_copy(grad_ref, rows_all.at[1, x, y], local.at[1]),
        pltpu.make_async_copy(win_ref, win, local.at[2]),
        pltpu.make_async_copy(wout_ref, wout, local.at[3]),
    ]
    for copy in stage:
        copy.start()
    barrier = pltpu.get_barrier_semaphore()
    for name, me, n in (("gx", x, nx), ("gy", y, ny), ("gz", z, nz)):
        for d in range(1, n):
            pl.semaphore_signal(
                barrier, inc=1, device_id={name: peer(me, d, n)}, device_id_type=MESH
            )
    pl.semaphore_wait(barrier, nx + ny + nz - 3)

    def across(arr, d):
        slot = rows_all.at[arr, x, source(y, d, ny)]
        for e in range(1, nx):
            send(slot, slot, a_x, (arr, e, d), {"gx": peer(x, e, nx)})

    for arr in range(2):
        stage[arr].wait()
        mine = rows_all.at[arr, x, y]
        for d in range(1, ny):
            send(mine, mine, a_z, (arr, d), {"gy": peer(y, d, ny)})
        across(arr, 0)

    def tiles(size, body):
        tile = 256 if size % 256 == 0 else 128

        def step(i, carry):
            body(pl.ds(pl.multiple_of(i * tile, tile), tile))
            return carry

        lax.fori_loop(0, size // tile, step, 0)

    def project(arr, e):
        left = rows_all.at[arr, block(e)]

        def body(cols):
            lhs = left[...].reshape(rows, width)
            if arr == 0:
                out = contract(lhs, win[:, cols], ((1,), (0,)))
            else:
                out = contract(lhs, wout[cols, :], ((1,), (1,)))
            part[arr, e, :, :, cols] = out.astype(BF16).reshape(nz, slab, -1)

        tiles(hidden, body)
        for d in range(1, nz):
            to = peer(z, d, nz)
            send(part.at[arr, e, to], part_in.at[arr, e, d], b_sem, (arr, e, d), {"gz": to})

    for arr in range(2):
        for d in range(1, ny):
            slot = rows_all.at[arr, x, source(y, d, ny)]
            remote(slot, slot, a_z, (arr, d), {"gy": y}).wait_recv()
            across(arr, d)
        stage[2 + arr].wait()
        project(arr, 0)

    def activate(e):
        for arr in range(2):
            for d in range(1, nz):
                got = part_in.at[arr, e, d]
                remote(got, got, b_sem, (arr, e, d), {"gz": z}).wait_recv()
        g = block(e)

        def body(cols):
            pre, d_act = part[0, e, z, :, cols].astype(F32), part[1, e, z, :, cols].astype(F32)
            for d in range(1, nz):
                pre = pre + part_in[0, e, d, :, cols].astype(F32)
                d_act = d_act + part_in[1, e, d, :, cols].astype(F32)
            cdf = 0.5 * (1.0 + lax.erf(pre * 0.7071067811865476))
            density = jnp.exp(-0.5 * pre * pre) * 0.3989422804014327
            hid_all[0, g, z, :, cols] = (pre * cdf).astype(BF16)
            hid_all[1, g, z, :, cols] = (d_act * (cdf + pre * density)).astype(BF16)

        tiles(hidden, body)
        for arr in range(2):
            mine = hid_all.at[arr, g, z]
            for d in range(1, nz):
                send(mine, mine, c_sem, (arr, e, d), {"gz": peer(z, d, nz)})

    for e in range(1, nx):
        for arr in range(2):
            for d in range(ny):
                slot = rows_all.at[arr, block(e), source(y, d, ny)]
                remote(slot, slot, a_x, (arr, e, d), {"gx": x}).wait_recv()
            project(arr, e)
    stores = [
        pltpu.make_async_copy(rows_all.at[0], tok_out, local.at[4]),
        pltpu.make_async_copy(rows_all.at[1], grad_out, local.at[5]),
    ]
    for copy in stores:
        copy.start()
    order = [*range(1, nx), 0]
    for e in [0, *range(1, nx)]:
        activate(e)

    def expand(arr, e, keep):
        g = block(e)
        for d in range(1, nz):
            got = hid_all.at[arr, g, source(z, d, nz)]
            remote(got, got, c_sem, (arr, e, d), {"gz": z}).wait_recv()
        left = hid_all.at[arr, g]

        def body(cols):
            lhs = left[...].reshape(rows, hidden)
            if arr == 0:
                out = contract(lhs, wout[:, cols], ((1,), (0,)))
            else:
                out = contract(lhs, win[cols, :], ((1,), (1,)))
            if keep:
                own[arr, :, :, cols] = out.reshape(ny, t, -1)
            else:
                send_out[arr, e, :, :, cols] = out.astype(BF16).reshape(ny, t, -1)

        tiles(width, body)
        if not keep:
            send(send_out.at[arr, e], fold_in.at[arr, e], d_x, (arr, e), {"gx": g})

    for e in order:
        for arr in range(2):
            expand(arr, e, e == 0)
    for arr, out in enumerate((act_out, dpre_out)):
        stores.append(pltpu.make_async_copy(hid_all.at[arr], out, local.at[6 + arr]))
        stores[-1].start()
    for arr in range(2):
        for e in range(1, nx):
            got = fold_in.at[arr, e]
            remote(got, got, d_x, (arr, e), {"gx": x}).wait_recv()

        def add(cols, arr=arr):
            total = own[arr, :, :, cols]
            for e in range(1, nx):
                total = total + fold_in[arr, e, :, :, cols].astype(F32)
            own[arr, :, :, cols] = total
            fold[arr, :, :, cols] = total.astype(BF16)

        tiles(width, add)
        for d in range(1, ny):
            to = peer(y, d, ny)
            send(fold.at[arr, to], last_in.at[arr, d], d_z, (arr, d), {"gy": to})
    for arr, out in enumerate((mlp_ref, tgrad_ref)):
        for d in range(1, ny):
            got = last_in.at[arr, d]
            remote(got, got, d_z, (arr, d), {"gy": y}).wait_recv()
        total = own[arr, y]
        for d in range(1, ny):
            total = total + last_in[arr, d].astype(F32)
        out[...] = total.astype(BF16)
    for copy in sends:
        copy.wait_send()
    for copy in stores:
        copy.wait()


def per_device(nx, ny, nz, tokens, grad_out, w_in, w_out):
    t, width = tokens.shape
    hidden = w_in.shape[1]
    rows = ny * t
    slab = rows // nz
    scale = 1.0 / math.sqrt(rows)
    anywhere = pl.BlockSpec(memory_space=pl.ANY)
    vmem = pl.BlockSpec(memory_space=pltpu.VMEM)
    dma = lambda *shape: pltpu.SemaphoreType.DMA((2, *shape))
    shape = jax.ShapeDtypeStruct
    mlp_out, tok_grad, tok_all, grad_all, act_all, d_pre_all = pl.pallas_call(
        functools.partial(ring_kernel, nx, ny, nz),
        out_shape=(
            shape((t, width), BF16), shape((t, width), BF16),
            shape((nx, ny, t, width), BF16), shape((nx, ny, t, width), BF16),
            shape((nx, nz, slab, hidden), BF16), shape((nx, nz, slab, hidden), BF16),
        ),
        in_specs=[anywhere] * 4,
        out_specs=(vmem, vmem, anywhere, anywhere, anywhere, anywhere),
        scratch_shapes=[
            pltpu.VMEM((2, nx, ny, t, width), BF16),
            pltpu.VMEM(w_in.shape, BF16),
            pltpu.VMEM(w_out.shape, BF16),
            pltpu.VMEM((2, nx, nz, slab, hidden), BF16),
            pltpu.VMEM((2, nx, nz, slab, hidden), BF16),
            pltpu.VMEM((2, nx, nz, slab, hidden), BF16),
            pltpu.VMEM((2, nx, ny, t, width), BF16),
            pltpu.VMEM((2, ny, t, width), F32),
            pltpu.VMEM((2, nx, ny, t, width), BF16),
            pltpu.VMEM((2, ny, t, width), BF16),
            pltpu.VMEM((2, ny, t, width), BF16),
            pltpu.SemaphoreType.DMA((8,)),
            dma(2, ny), dma(2, nx, ny), dma(2, nx, nz), dma(2, nx, nz), dma(2, nx), dma(2, ny),
        ],
        compiler_params=pltpu.CompilerParams(
            collective_id=0, has_side_effects=True, vmem_limit_bytes=60 * 2**20
        ),
    )(tokens, grad_out, w_in, w_out)
    tok_all, grad_all = tok_all.reshape(-1, width), grad_all.reshape(-1, width)
    act_all, d_pre_all = act_all.reshape(-1, hidden), d_pre_all.reshape(-1, hidden)
    wout_grad = contract(act_all, grad_all, ((0,), (0,))) * scale
    win_grad = contract(tok_all, d_pre_all, ((0,), (0,))) * scale
    return mlp_out, tok_grad, win_grad, wout_grad


def solution(mesh):
    rows_spec = P(("gx", "gy"), "gz")
    in_spec = P("gz", ("gy", "gx"))
    out_spec = P(("gy", "gx"), "gz")
    sizes = (mesh.shape["gx"], mesh.shape["gy"], mesh.shape["gz"])
    return jax.shard_map(
        functools.partial(per_device, *sizes),
        mesh=mesh,
        in_specs=(rows_spec, rows_spec, in_spec, out_spec),
        out_specs=(rows_spec, rows_spec, in_spec, out_spec),
        check_vma=False,
    )
```

```python
import functools
import math

import jax
import jax.numpy as jnp
from jax import lax
from jax.experimental import pallas as pl
from jax.experimental.pallas import tpu as pltpu
from jax.sharding import PartitionSpec as P

MESH = pl.DeviceIdType.MESH
F32, BF16 = jnp.float32, jnp.bfloat16


def contract(left, right, dims):
    return lax.dot_general(left, right, (dims, ((), ())), preferred_element_type=F32)


def ring_kernel(
    nx, ny, nz,
    tok_ref, grad_ref, win_ref, wout_ref,
    mlp_ref, tgrad_ref, tok_out, grad_out, act_out, dpre_out,
    rows_all, win, wout, part, pair_in, paired, part_in, hid_all, send_out, own, fold_in, fold, last_in,
    local, a_z, a_x, p_sem, b_sem, c_sem, d_x, d_z,
):
    x, y, z = lax.axis_index("gx"), lax.axis_index("gy"), lax.axis_index("gz")
    t, width = tok_ref.shape
    hidden = win_ref.shape[1]
    rows = ny * t
    slab = rows // nz
    half = nz // 2
    core, chip = lax.rem(z, 2), lax.div(z, 2)
    partner = z + 1 - 2 * core
    mine_at = core * half + chip
    sends = []

    def block(e):
        return lax.rem(x - e + nx, nx)

    def peer(me, d, n):
        return lax.rem(me + d, n)

    def source(me, d, n):
        return lax.rem(me - d + n, n)

    def remote(src, dst, sems, index, device):
        return pltpu.make_async_remote_copy(
            src_ref=src, dst_ref=dst, send_sem=sems.at[(0, *index)],
            recv_sem=sems.at[(1, *index)], device_id=device, device_id_type=MESH,
        )

    def send(*args):
        copy = remote(*args)
        copy.start()
        sends.append(copy)

    stage = [
        pltpu.make_async_copy(tok_ref, rows_all.at[0, x, y], local.at[0]),
        pltpu.make_async_copy(grad_ref, rows_all.at[1, x, y], local.at[1]),
        pltpu.make_async_copy(win_ref, win, local.at[2]),
        pltpu.make_async_copy(wout_ref, wout, local.at[3]),
    ]
    for copy in stage:
        copy.start()
    barrier = pltpu.get_barrier_semaphore()
    for name, me, n in (("gx", x, nx), ("gy", y, ny), ("gz", z, nz)):
        for d in range(1, n):
            pl.semaphore_signal(
                barrier, inc=1, device_id={name: peer(me, d, n)}, device_id_type=MESH
            )
    pl.semaphore_wait(barrier, nx + ny + nz - 3)

    def across(arr, d):
        slot = rows_all.at[arr, x, source(y, d, ny)]
        for e in range(1, nx):
            send(slot, slot, a_x, (arr, e, d), {"gx": peer(x, e, nx)})

    for arr in range(2):
        stage[arr].wait()
        mine = rows_all.at[arr, x, y]
        for d in range(1, ny):
            send(mine, mine, a_z, (arr, d), {"gy": peer(y, d, ny)})
        across(arr, 0)

    def tiles(size, body, base=0):
        tile = 256 if size % 256 == 0 else 128

        def step(i, carry):
            body(pl.ds(pl.multiple_of(base + i * tile, 128), tile))
            return carry

        lax.fori_loop(0, size // tile, step, 0)

    def project(arr, e):
        left = rows_all.at[arr, block(e)]

        def body(cols):
            lhs = left[...].reshape(rows, width)
            if arr == 0:
                out = contract(lhs, win[:, cols], ((1,), (0,)))
            else:
                out = contract(lhs, wout[cols, :], ((1,), (1,)))
            part[arr, e, :, :, cols] = out.astype(BF16).reshape(nz, slab, -1)

        tiles(hidden, body)
        got = pair_in.at[arr, e]
        theirs = part.at[arr, e, pl.ds((1 - core) * half, half)]
        send(theirs, got, p_sem, (arr, e), {"gz": partner})
        remote(got, got, p_sem, (arr, e), {"gz": z}).wait_recv()

        def join(cols):
            for d in range(half):
                total = part[arr, e, core * half + d, :, cols].astype(F32)
                total = total + pair_in[arr, e, d, :, cols].astype(F32)
                paired[arr, e, d, :, cols] = total.astype(BF16)

        tiles(hidden, join)
        for d in range(1, half):
            to = peer(chip, d, half)
            send(
                paired.at[arr, e, to], part_in.at[arr, e, d], b_sem, (arr, e, d),
                {"gz": 2 * to + core},
            )

    for arr in range(2):
        for d in range(1, ny):
            slot = rows_all.at[arr, x, source(y, d, ny)]
            remote(slot, slot, a_z, (arr, d), {"gy": y}).wait_recv()
            across(arr, d)
        stage[2 + arr].wait()
        project(arr, 0)

    def activate(e):
        for arr in range(2):
            for d in range(1, half):
                got = part_in.at[arr, e, d]
                remote(got, got, b_sem, (arr, e, d), {"gz": z}).wait_recv()
        g = block(e)

        def body(cols):
            pre = paired[0, e, chip, :, cols].astype(F32)
            d_act = paired[1, e, chip, :, cols].astype(F32)
            for d in range(1, half):
                pre = pre + part_in[0, e, d, :, cols].astype(F32)
                d_act = d_act + part_in[1, e, d, :, cols].astype(F32)
            cdf = 0.5 * (1.0 + lax.erf(pre * 0.7071067811865476))
            density = jnp.exp(-0.5 * pre * pre) * 0.3989422804014327
            hid_all[0, g, mine_at, :, cols] = (pre * cdf).astype(BF16)
            hid_all[1, g, mine_at, :, cols] = (d_act * (cdf + pre * density)).astype(BF16)

        tiles(hidden, body)
        for arr in range(2):
            mine = hid_all.at[arr, g, mine_at]
            for d in range(1, half):
                to = peer(chip, d, half)
                send(mine, mine, c_sem, (arr, e, d), {"gz": 2 * to + core})
            send(mine, mine, c_sem, (arr, e, 0), {"gz": partner})

    def relay(arr, e):
        for d in range(1, half):
            slot = hid_all.at[arr, block(e), core * half + source(chip, d, half)]
            remote(slot, slot, c_sem, (arr, e, d), {"gz": z}).wait_recv()
            send(slot, slot, c_sem, (arr, e, half - 1 + d), {"gz": partner})

    for e in range(1, nx):
        for arr in range(2):
            for d in range(ny):
                slot = rows_all.at[arr, block(e), source(y, d, ny)]
                remote(slot, slot, a_x, (arr, e, d), {"gx": x}).wait_recv()
            project(arr, e)
    stores = [
        pltpu.make_async_copy(rows_all.at[0], tok_out, local.at[4]),
        pltpu.make_async_copy(rows_all.at[1], grad_out, local.at[5]),
    ]
    for copy in stores:
        copy.start()
    order = [*range(1, nx), 0]
    for e in [0, *range(1, nx)]:
        activate(e)
    for e in order:
        for arr in range(2):
            relay(arr, e)

    def expand(arr, e, keep):
        g = block(e)
        for d in range(half):
            got = hid_all.at[arr, g, (1 - core) * half + source(chip, d, half)]
            index = half - 1 + d if d else 0
            remote(got, got, c_sem, (arr, e, index), {"gz": z}).wait_recv()
        left = hid_all.at[arr, g]

        def body(cols):
            lhs = left[...].reshape(rows, hidden)
            if arr == 0:
                out = contract(lhs, wout[:, cols], ((1,), (0,)))
            else:
                out = contract(lhs, win[cols, :], ((1,), (1,)))
            if keep:
                own[arr, :, :, cols] = out.reshape(ny, t, -1)
            else:
                send_out[arr, e, :, :, cols] = out.astype(BF16).reshape(ny, t, -1)

        for q in range(2):
            view = pl.ds(q * (width // 2), width // 2)
            tiles(width // 2, body, q * (width // 2))
            if not keep:
                send(
                    send_out.at[arr, e, :, :, view], fold_in.at[arr, e, :, :, view],
                    d_x, (arr, e, q), {"gx": g},
                )

    for e in order:
        for arr in range(2):
            expand(arr, e, e == 0)
    for arr, out in enumerate((act_out, dpre_out)):
        stores.append(pltpu.make_async_copy(hid_all.at[arr], out, local.at[6 + arr]))
        stores[-1].start()
    def add(arr, cols):
        total = own[arr, :, :, cols]
        for e in range(1, nx):
            total = total + fold_in[arr, e, :, :, cols].astype(F32)
        own[arr, :, :, cols] = total
        fold[arr, :, :, cols] = total.astype(BF16)

    for arr in range(2):
        for q in range(2):
            view = pl.ds(q * (width // 2), width // 2)
            for e in range(1, nx):
                got = fold_in.at[arr, e, :, :, view]
                remote(got, got, d_x, (arr, e, q), {"gx": x}).wait_recv()
            tiles(width // 2, functools.partial(add, arr), q * (width // 2))
            for d in range(1, ny):
                to = peer(y, d, ny)
                send(
                    fold.at[arr, to, :, view], last_in.at[arr, d, :, view],
                    d_z, (arr, d, q), {"gy": to},
                )
    for arr, out in enumerate((mlp_ref, tgrad_ref)):
        for d in range(1, ny):
            for q in range(2):
                got = last_in.at[arr, d, :, pl.ds(q * (width // 2), width // 2)]
                remote(got, got, d_z, (arr, d, q), {"gy": y}).wait_recv()
        total = own[arr, y]
        for d in range(1, ny):
            total = total + last_in[arr, d].astype(F32)
        out[...] = total.astype(BF16)
    for copy in sends:
        copy.wait_send()
    for copy in stores:
        copy.wait()


def per_device(nx, ny, nz, tokens, grad_out, w_in, w_out):
    t, width = tokens.shape
    hidden = w_in.shape[1]
    rows = ny * t
    slab = rows // nz
    scale = 1.0 / math.sqrt(rows)
    anywhere = pl.BlockSpec(memory_space=pl.ANY)
    vmem = pl.BlockSpec(memory_space=pltpu.VMEM)
    dma = lambda *shape: pltpu.SemaphoreType.DMA((2, *shape))
    shape = jax.ShapeDtypeStruct
    mlp_out, tok_grad, tok_all, grad_all, act_all, d_pre_all = pl.pallas_call(
        functools.partial(ring_kernel, nx, ny, nz),
        out_shape=(
            shape((t, width), BF16), shape((t, width), BF16),
            shape((nx, ny, t, width), BF16), shape((nx, ny, t, width), BF16),
            shape((nx, nz, slab, hidden), BF16), shape((nx, nz, slab, hidden), BF16),
        ),
        in_specs=[anywhere] * 4,
        out_specs=(vmem, vmem, anywhere, anywhere, anywhere, anywhere),
        scratch_shapes=[
            pltpu.VMEM((2, nx, ny, t, width), BF16),
            pltpu.VMEM(w_in.shape, BF16),
            pltpu.VMEM(w_out.shape, BF16),
            pltpu.VMEM((2, nx, nz, slab, hidden), BF16),
            pltpu.VMEM((2, nx, nz // 2, slab, hidden), BF16),
            pltpu.VMEM((2, nx, nz // 2, slab, hidden), BF16),
            pltpu.VMEM((2, nx, nz // 2, slab, hidden), BF16),
            pltpu.VMEM((2, nx, nz, slab, hidden), BF16),
            pltpu.VMEM((2, nx, ny, t, width), BF16),
            pltpu.VMEM((2, ny, t, width), F32),
            pltpu.VMEM((2, nx, ny, t, width), BF16),
            pltpu.VMEM((2, ny, t, width), BF16),
            pltpu.VMEM((2, ny, t, width), BF16),
            pltpu.SemaphoreType.DMA((8,)),
            dma(2, ny), dma(2, nx, ny), dma(2, nx), dma(2, nx, nz), dma(2, nx, nz), dma(2, nx, 2), dma(2, ny, 2),
        ],
        compiler_params=pltpu.CompilerParams(
            collective_id=0, has_side_effects=True, vmem_limit_bytes=60 * 2**20
        ),
    )(tokens, grad_out, w_in, w_out)
    tok_all, grad_all = tok_all.reshape(-1, width), grad_all.reshape(-1, width)
    act_all, d_pre_all = act_all.reshape(-1, hidden), d_pre_all.reshape(-1, hidden)
    wout_grad = contract(act_all, grad_all, ((0,), (0,))) * scale
    win_grad = contract(tok_all, d_pre_all, ((0,), (0,))) * scale
    return mlp_out, tok_grad, win_grad, wout_grad


def solution(mesh):
    rows_spec = P(("gx", "gy"), "gz")
    in_spec = P("gz", ("gy", "gx"))
    out_spec = P(("gy", "gx"), "gz")
    sizes = (mesh.shape["gx"], mesh.shape["gy"], mesh.shape["gz"])
    return jax.shard_map(
        functools.partial(per_device, *sizes),
        mesh=mesh,
        in_specs=(rows_spec, rows_spec, in_spec, out_spec),
        out_specs=(rows_spec, rows_spec, in_spec, out_spec),
        check_vma=False,
    )
```
